256 devices in a mesh: seq: 2 (over core), batch: 128 (over z, y, x).
Axes of the slice: x: 4, y: 4, z: 8, core: 2. Of those that a mesh axis runs over, the one named last changes fastest.
Arguments:
- queries: bfloat16 [128, 1024, 1024], P('batch', 'seq'), may hold values from -6 to 6
- keys: bfloat16 [128, 1024, 1024], P('batch', 'seq'), may hold values from -6 to 6
- values: bfloat16 [128, 1024, 2048], P('batch', 'seq'), may hold values from -6 to 6
- gate_rate: bfloat16 [128, 1024, 1024], P('batch', 'seq'), may hold values from 0.5 to 2
- segment_ids: int32 [128, 1024], P('batch', 'seq'), may hold values from 0 to 2, never falling along the last dimension, each value on 1 to 512 neighbouring positions
- decay_exps: int32 [4], replicated, may hold values from 0 to 13
- out_weight: bfloat16 [2048, 2048], P('batch'), may hold values from -0.125 to 0.125
Outputs:
- projected: bfloat16 [128, 1024, 2048], P('batch', 'seq')
The draws below stay inside these ranges and needn't reach their ends.
Inputs may be any that keep to these rules, and one draw needn't show every extreme that they name: `segment_ids`: within each stream the ids never fall and start at 0; each of the 3 ids covers 1 to 512 consecutive tokens, one of them exactly 512.
All inputs are finite; a program needn't handle non-finite values.
Results may differ from the reference program's by a relative error of at most 0.004.
The reference program's roundings to bfloat16 on the way (of `hidden`) count: a program that leaves them out, or rounds other values in their place, can miss the bound.
Values may be sent and summed in bfloat16 or wider, within the bound.
A program may use at most 128 MiB of HBM per device.

```python
import math
import jax
import jax.numpy as jnp
import numpy as np
from jax import lax

D = 2048
HEADS = 4
HEAD_K = 256
BLOCK = 64
SEGS = 3
SEQLEN = 1024
GROUPS = 128
KEYS = 1024
VALS = 2048


def place_ends(values, own_key, low, top_value):
    longest = values.shape.index(max(values.shape))
    spots = []
    for shift in (0, 1):
        where = [jax.random.randint(jax.random.fold_in(own_key, axis), (), 0, length) for axis, length in enumerate(values.shape)]
        where[longest] = (where[longest] + shift) % values.shape[longest]
        spots.append(tuple(where))
    return values.at[spots[0]].set(low).at[spots[1]].set(top_value)


def steps_of(rng, extent, cuts, low, top_value):
    def one(position, blocks):
        draws = jax.random.uniform(jax.random.fold_in(jax.random.fold_in(rng, 6), position), (blocks,), jnp.float32, low / len(cuts), top_value / len(cuts))
        return jnp.repeat(jnp.exp(draws), extent[position] // blocks).reshape((-1,) + (1,) * (len(extent) - position - 1))

    level = one(*cuts[0])
    for cut in cuts[1:]:
        level = level * one(*cut)
    return level


def profile(count, total, reach, skew):
    portions = [(1 << 20) // math.isqrt(standing ** skew) + 1 for standing in range(2, count + 1)]
    surplus, holding = total - reach - (count - 1), [1] * (count - 1)
    while surplus > 0:
        movable = [i for i in range(count - 1) if holding[i] < reach]
        pool, remaining = sum([portions[i] for i in movable]), surplus
        for i in movable:
            extra = min(reach - holding[i], max(1, remaining * portions[i] // pool), surplus)
            holding[i] = holding[i] + extra
            surplus = surplus - extra
    return np.array([reach] + holding)


def ragged(own_key, number_of, total, most, skew):
    if number_of == 2:
        one = jax.random.randint(own_key, (), max(1, total - most), min(most, total - 1) + 1)
        return jnp.stack([one, total - one])
    sizes = jnp.asarray(profile(number_of, total, most, skew), jnp.int32)
    pairs = (number_of - 1) // 2
    giver, taker = sizes[1:1 + 2 * pairs:2], sizes[2:2 + 2 * pairs:2]
    margin = jnp.minimum(giver - 1, most - taker)
    shifted = jax.random.randint(jax.random.fold_in(own_key, 1), (pairs,), 0, 1 << 20) % (margin + 1)
    sizes = sizes.at[1:1 + 2 * pairs:2].set(giver - shifted).at[2:2 + 2 * pairs:2].set(taker + shifted)
    return sizes[jax.random.permutation(jax.random.fold_in(own_key, 2), number_of)]


def centred(stream_key, shape, scale, limit, cuts=(), kind=jnp.bfloat16):
    values = jax.random.normal(stream_key, shape, jnp.float32) * scale
    if len(cuts) > 0:
        values = steps_of(stream_key, shape, cuts, -0.22, 0.18) * values
    return jnp.clip(values, min=-limit, max=limit).astype(kind)


def setup_inputs(seed: int = 0) -> dict:
    arg_keys = jax.random.split(jax.random.key(seed), 8)
    return {
        "queries": centred(arg_keys[0], (GROUPS, SEQLEN, KEYS), 1.0, 6.0, ((0, 128), (1, 2))),
        "keys": centred(arg_keys[1], (GROUPS, SEQLEN, KEYS), 1.0, 6.0, ((0, 128), (1, 2))),
        "values": centred(arg_keys[2], (GROUPS, SEQLEN, VALS), 1.0, 6.0, ((0, 128), (1, 2))),
        "gate_rate": jnp.clip(jnp.exp(math.log(2.0) - 1.3862944 * jax.random.uniform(arg_keys[3], (GROUPS, SEQLEN, KEYS), jnp.float32) ** steps_of(arg_keys[3], (GROUPS, SEQLEN, KEYS), ((0, 128), (1, 2)), -0.2, 0.2)), 0.5, 2.0).astype(jnp.bfloat16),
        "segment_ids": jax.vmap(lambda own: jnp.searchsorted(jnp.cumsum(ragged(own, SEGS, SEQLEN, SEQLEN // 2, 2)), jnp.arange(SEQLEN), side="right"))(jax.random.split(arg_keys[4], GROUPS)).reshape((GROUPS, SEQLEN)).astype(jnp.int32),
        "decay_exps": place_ends(jax.random.randint(arg_keys[5], (HEADS,), 0, 14), jax.random.fold_in(arg_keys[5], 1), 0, 13).astype(jnp.int32),
        "out_weight": centred(arg_keys[6], (VALS, D), VALS ** -0.5, 0.125, ((0, 128),)),
    }


def linear_blocks(lifted_query, key_heads, value_heads, log_decay, starts, initial):
    groups, length, head_count, key_width = lifted_query.shape
    value_width = value_heads.shape[3]
    block_count = length // BLOCK

    def split(member):
        return jnp.swapaxes(member.reshape((groups, block_count, BLOCK) + member.shape[2:]), 0, 1)

    def advance(carried, pieces):
        query_rows, key_rows, value_rows, log_rows, start_rows = pieces
        running = jnp.cumsum(log_rows, axis=1)
        segment_rank = jnp.cumsum(start_rows, axis=1)
        unbroken = (segment_rank == 0).astype(jnp.float32)
        raised_q = query_rows * jnp.exp(running)
        raised_k = key_rows * jnp.exp(-running)
        scores = jnp.einsum('gthc,gshc->ghts', raised_q, raised_k, precision=lax.Precision.HIGHEST)
        order = jnp.arange(BLOCK)
        causal = order[:, None] >= order[None, :]
        same_doc = segment_rank[:, :, None] == segment_rank[:, None, :]
        allowed = jnp.logical_and(causal[None], same_doc).astype(jnp.float32)
        inside = jnp.einsum('ghts,gshv->gthv', scores * allowed[:, None], value_rows, precision=lax.Precision.HIGHEST)
        outside = unbroken[:, :, None, None] * jnp.einsum('gthc,ghcv->gthv', raised_q, carried, precision=lax.Precision.HIGHEST)
        final_log = running[:, -1]
        in_last = (segment_rank == segment_rank[:, -1:]).astype(jnp.float32)
        weighted = key_rows * jnp.exp(final_log[:, None] - running) * in_last[:, :, None, None]
        kept = unbroken[:, -1][:, None, None, None] * jnp.exp(final_log)[..., None] * carried
        updated = kept + jnp.einsum('gshc,gshv->ghcv', weighted, value_rows, precision=lax.Precision.HIGHEST)
        return (updated, inside + outside)
    members = (lifted_query, key_heads, value_heads, log_decay, starts)
    final, outputs = lax.scan(advance, initial, tuple((split(member) for member in members)))
    outputs = jnp.swapaxes(outputs, 0, 1).reshape(groups, length, head_count, value_width)
    return (outputs, final)

def reference(queries, keys, values, gate_rate, segment_ids, decay_exps, out_weight):
    groups = queries.shape[0]
    length = queries.shape[1]
    head_count = decay_exps.shape[0]

    def heads_of(array):
        return array.astype(jnp.float32).reshape(groups, length, head_count, -1)
    scaling = jnp.exp2(-decay_exps.astype(jnp.float32)) / 16.0
    log_decay = -heads_of(gate_rate) * scaling[None, None, :, None]
    previous = jnp.concatenate([jnp.full((groups, 1), -1, jnp.int32), segment_ids[:, :-1]], axis=1)
    starts = (segment_ids != previous).astype(jnp.float32)
    query_heads = heads_of(queries) * (1.0 / math.sqrt(HEAD_K))
    key_heads = heads_of(keys)
    value_heads = heads_of(values)
    initial = jnp.zeros((groups, head_count, key_heads.shape[3], value_heads.shape[3]), jnp.float32)
    mixed, final = linear_blocks(query_heads, key_heads, value_heads, log_decay, starts, initial)
    normed = mixed / jnp.sqrt(lax.optimization_barrier(jnp.mean(mixed * mixed, axis=-1, keepdims=True)) + 1.0)
    hidden = normed.astype(jnp.bfloat16).reshape(groups * length, -1)
    product = jnp.dot(hidden, out_weight, preferred_element_type=jnp.float32)
    return product.astype(jnp.bfloat16).reshape(groups, length, -1)
```

```python
import functools
import math

import jax
import jax.numpy as jnp
from jax import lax
from jax.experimental import pallas as pl
from jax.experimental.pallas import tpu as pltpu
from jax.sharding import Mesh
from jax.sharding import PartitionSpec as P

BLOCK = 256
F32, BF16 = jnp.float32, jnp.bfloat16


def halves(x):
    high = x.astype(BF16)
    return high, (x - high.astype(F32)).astype(BF16)


def dot(a, b, dims):
    return lax.dot_general(a, b, (dims, ((), ())), preferred_element_type=F32)


def decay_rate(decay_ref, h, width):
    exponent = jnp.full((1, width), decay_ref[h], jnp.int32).astype(F32)
    return -(jnp.exp2(-exponent) / 16.0)


def running_log(gate, rate):
    rows = lax.broadcasted_iota(jnp.int32, (BLOCK, BLOCK), 0)
    cols = lax.broadcasted_iota(jnp.int32, (BLOCK, BLOCK), 1)
    triangle = jnp.where(rows >= cols, 1.0, 0.0).astype(BF16)
    parts, carry = [], None
    for b in range(gate.shape[0] // BLOCK):
        part = dot(triangle, gate[b * BLOCK : (b + 1) * BLOCK], ((1,), (0,)))
        if carry is not None:
            part = part + carry
        carry = part[BLOCK - 1 :]
        parts.append(part)
    return jnp.concatenate(parts, axis=0) * rate


def column(row, width):
    return jnp.transpose(jnp.broadcast_to(row, (width, row.shape[1])))


def state_of(k, v, log, same):
    weight = k.astype(F32) * jnp.exp(log[-1:] - log) * same
    high, low = halves(weight)
    return dot(jnp.concatenate([high, low], axis=0), jnp.concatenate([v, v], axis=0), ((0,), (0,)))


def inside(q_high, q_low, k_high, k_low, v, seg_row, seg_col, b):
    here, upto = b * BLOCK, (b + 1) * BLOCK
    qh, ql = q_high[here:upto], q_low[here:upto]
    kh, kl = k_high[:upto], k_low[:upto]
    scores = dot(
        jnp.concatenate([qh, qh, ql], axis=1), jnp.concatenate([kh, kl, kh], axis=1), ((1,), (1,))
    )
    rows = lax.broadcasted_iota(jnp.int32, scores.shape, 0) + here
    cols = lax.broadcasted_iota(jnp.int32, scores.shape, 1)
    seg_t = jnp.concatenate([seg_col[here:upto]] * (upto // 128), axis=1)
    allowed = jnp.logical_and(rows >= cols, seg_t == seg_row[:, :upto])
    high, low = halves(jnp.where(allowed, scores, 0.0))
    return dot(
        jnp.concatenate([high, low], axis=1), jnp.concatenate([v[:upto], v[:upto]], axis=0), ((1,), (0,))
    )


def state_kernel(key_width, value_width, heads, decay_ref, seg_ref, k_ref, g_ref, v_ref, s_ref):
    @pl.when(lax.axis_index("seq") == 0)
    def _():
        seg_col = column(seg_ref[...].astype(F32), 128)
        same = (seg_col == seg_col[-1:]).astype(F32)
        same = jnp.concatenate([same] * (key_width // 128), axis=1)
        for h in range(heads):
            ks, vs = pl.ds(h * key_width, key_width), pl.ds(h * value_width, value_width)
            log = running_log(g_ref[:, ks], decay_rate(decay_ref, h, key_width))
            s_ref[h] = state_of(k_ref[:, ks], v_ref[:, vs], log, same)


def mix_kernel(key_width, value_width, heads, decay_ref, prior_ref, seg_ref, q_ref, k_ref, g_ref, v_ref, s_ref, o_ref):
    seg_row = seg_ref[...].astype(F32)
    seg_col = column(seg_row, 128)
    going = (seg_col == prior_ref[...].astype(F32)).astype(F32)
    going = jnp.concatenate([going] * (value_width // 128), axis=1)
    for h in range(heads):
        ks, vs = pl.ds(h * key_width, key_width), pl.ds(h * value_width, value_width)
        log = running_log(g_ref[:, ks], decay_rate(decay_ref, h, key_width))
        q_high, q_low = halves(q_ref[:, ks].astype(F32) * (1.0 / math.sqrt(key_width)) * jnp.exp(log))
        k_high, k_low = halves(k_ref[:, ks].astype(F32) * jnp.exp(-log))
        v = v_ref[:, vs]
        mixed = jnp.concatenate(
            [
                inside(q_high, q_low, k_high, k_low, v, seg_row, seg_col, b)
                for b in range(q_high.shape[0] // BLOCK)
            ],
            axis=0,
        )
        s_high, s_low = halves(s_ref[h])
        mixed = mixed + going * dot(
            jnp.concatenate([q_high, q_high, q_low], axis=1),
            jnp.concatenate([s_high, s_low, s_high], axis=0),
            ((1,), (0,)),
        )
        square = jnp.sum(mixed * mixed, axis=1, keepdims=True) * (1.0 / value_width)
        o_ref[:, vs] = (mixed / jnp.sqrt(square + 1.0)).astype(BF16)


def local(queries, keys, values, gate_rate, segment_ids, decay_exps, out_weight):
    length, heads = queries.shape[1], decay_exps.shape[0]
    key_width, value_width = queries.shape[2] // heads, values.shape[2] // heads
    q, k, g, v = queries[0], keys[0], gate_rate[0], values[0]
    whole = pl.BlockSpec(memory_space=pltpu.VMEM)
    scalar = pl.BlockSpec(memory_space=pltpu.SMEM)
    params = pltpu.CompilerParams(vmem_limit_bytes=60 * 1024 * 1024)
    weight = lax.all_gather(out_weight, ("batch_0", "batch_1", "batch_2"), axis=0, tiled=True)
    state = pl.pallas_call(
        functools.partial(state_kernel, key_width, value_width, heads),
        out_shape=jax.ShapeDtypeStruct((heads, key_width, value_width), F32),
        in_specs=[scalar] + [whole] * 4,
        out_specs=whole,
        compiler_params=params,
        name="state",
    )(decay_exps, segment_ids, k, g, v)
    incoming = lax.ppermute(state, "seq", [(0, 1)])
    prior = lax.ppermute(segment_ids[:, -1:] + 1, "seq", [(0, 1)]) - 1
    hidden = pl.pallas_call(
        functools.partial(mix_kernel, key_width, value_width, heads),
        out_shape=jax.ShapeDtypeStruct((length, heads * value_width), BF16),
        in_specs=[scalar] + [whole] * 7,
        out_specs=whole,
        compiler_params=params,
        name="mix",
    )(decay_exps, prior, segment_ids, q, k, g, v, incoming)
    product = jnp.dot(hidden, weight, preferred_element_type=F32)
    return product.astype(BF16)[None]


def solution(mesh):
    split = Mesh(
        mesh.devices.reshape(mesh.shape["seq"], 8, 4, 4), ("seq", "batch_0", "batch_1", "batch_2")
    )
    batch = ("batch_0", "batch_1", "batch_2")
    return jax.shard_map(
        local,
        mesh=split,
        in_specs=(P(batch, "seq", None),) * 4 + (P(batch, "seq"), P(), P(batch, None)),
        out_specs=P(batch, "seq", None),
        check_vma=False,
    )
```
